32 devices in a mesh: batch: 2 (over x), items: 16 (over z, y, core).
Axes of the slice: x: 2, y: 2, z: 4, core: 2. Of those that a mesh axis runs over, the one named last changes fastest.
Arguments:
- users: bfloat16 [1280, 256], P(('batch', 'items')), may hold values from -6 to 6
- items: bfloat16 [8192, 256], P(('batch', 'items')), may hold values from -6 to 6
- pos_ids: int32 [1280], P(('batch', 'items')), may hold values from 0 to 8191
Outputs:
- loss: float32 [1280], P(('batch', 'items'))
- user_grad: float32 [1280, 256], P(('batch', 'items'))
- item_grad: float32 [8192, 256], P(('batch', 'items'))
The draws below stay inside these ranges and needn't reach their ends.
All inputs are finite; a program needn't handle non-finite values.
Results may differ from the reference program's by a relative error of at most 0.0015.
Values may be sent and summed in bfloat16 or wider, within the bound.
No kernel may reach another device: no remote copies, remote signals or barrier semaphores. Data moves between devices by JAX's collectives and lax.ppermute only.
A program may use at most 64 MiB of HBM per device.

```python
import math
import jax
import jax.numpy as jnp
from jax import lax

E = 256
USERS = 1280
ITEMS = 8192


def joint_towers(key):
    base = jax.random.fold_in(key, 7)
    key_user, key_item, key_pick, key_flag, key_sign, key_align, key_perm = jax.random.split(base, 7)
    users = jnp.clip(jax.random.normal(key_user, (USERS, E), jnp.float32), -6.0, 6.0)
    bank = jnp.clip(0.125 * jax.random.normal(key_item, (ITEMS, E), jnp.float32), -0.75, 0.75)
    user_level = 5.0
    item_level = 320.0 / (user_level * E)
    signs = (2 * jax.random.randint(key_sign, (USERS, E), 0, 2) - 1).astype(jnp.float32)
    aligned = jax.random.randint(key_align, (USERS,), 0, 16) == 0
    users = jnp.where(aligned[:, None], user_level * signs, users)
    users = users.astype(jnp.bfloat16).astype(jnp.float32)
    order = jax.random.permutation(key_perm, ITEMS).astype(jnp.int32)
    rank = jnp.argsort(order).astype(jnp.int32)
    owned = rank < USERS
    partner = jnp.minimum(rank, USERS - 1)
    match = owned & aligned[partner]
    bank = jnp.where(match[:, None], item_level * signs[partner], bank)
    return (users, bank)


def draw_users(key, part):
    return joint_towers(key)[0].astype(jnp.bfloat16)


def draw_items(key, part):
    return joint_towers(key)[1].astype(jnp.bfloat16)


def place_ends(drawn, stream_key, least, high):
    dims = drawn.shape
    index_at = [jax.random.randint(jax.random.fold_in(stream_key, axis), (), 0, dims[axis]) for axis in range(len(dims))]
    drawn = drawn.at[tuple(index_at)].set(least)
    longest = dims.index(max(dims))
    index_at[longest] = (index_at[longest] + 1) % dims[longest]
    return drawn.at[tuple(index_at)].set(high)


def setup_inputs(seed: int = 0) -> dict:
    keys = jax.random.split(jax.random.key(seed), 4)
    return {
        "users": draw_users(jax.random.fold_in(keys[3], 71), 0),
        "items": draw_items(jax.random.fold_in(keys[3], 71), 0),
        "pos_ids": place_ends(jax.random.randint(keys[2], (USERS,), 0, ITEMS), jax.random.fold_in(keys[2], 1), 0, ITEMS - 1).astype(jnp.int32),
    }


def reference(users, items, pos_ids):
    rows = users.shape[0]
    size = math.gcd(rows, 1024)
    count = rows // size
    bank = items.astype(jnp.float32)
    cols = jnp.arange(items.shape[0], dtype=jnp.int32)

    def step(carry, args):
        ublk, pblk = args
        user_block = ublk.astype(jnp.float32)
        logit = jnp.dot(user_block, bank.T, precision=lax.Precision.HIGHEST)
        mask = pblk[:, None] == cols[None, :]
        peak = jnp.max(logit, axis=1)
        total = jnp.sum(jnp.exp(logit - peak[:, None]), axis=1)
        lse = peak + jnp.log(total)
        positive = jnp.sum(jnp.where(mask, logit, jnp.float32(0.0)), axis=1)
        weights = (jnp.exp(logit - lse[:, None]) - mask.astype(jnp.float32)).astype(jnp.bfloat16)
        weight_full = weights.astype(jnp.float32)
        ugrad = jnp.dot(weight_full, bank, precision=lax.Precision.HIGHEST)
        carry = carry + jnp.dot(weight_full.T, user_block, precision=lax.Precision.HIGHEST)
        return carry, (lse - positive, ugrad)

    start = jnp.zeros(items.shape, jnp.float32)
    item_grad, outputs = lax.scan(step, start, (users.reshape(count, size, users.shape[1]), pos_ids.reshape(count, size)))
    loss = outputs[0].reshape(rows)
    user_grad = outputs[1].reshape(rows, users.shape[1])
    return (loss, user_grad, item_grad)
```

```python
import jax
import jax.numpy as jnp
from jax import lax
from jax.sharding import PartitionSpec as P


def swap(value, axis, mask):
    count = lax.axis_size(axis)
    return lax.ppermute(value, axis, [(i, i ^ mask) for i in range(count)])


def user_steps(count):
    bits = [1 << k for k in range(count.bit_length() - 1)][1:]
    steps = [(b, b) for b in bits[1:]]
    if len(steps) > 1:
        steps[-1] = (bits[-1], bits[-1] | bits[-2])
    return steps + [(b, b) for b in bits[:1]]


def doubled(mine, theirs, upper):
    return jnp.where(
        upper, jnp.concatenate([theirs, mine], 0), jnp.concatenate([mine, theirs], 0)
    )


def local(users, items, pos_ids):
    f32, bf16 = jnp.float32, jnp.bfloat16
    own, width = users.shape
    per_bank = items.shape[0]
    count = lax.axis_size("items")
    here = lax.axis_index("items")
    group = lax.axis_index("batch")
    steps = user_steps(count)
    block = -(-(own + 1) // 16) * 16

    ids_row = jnp.concatenate(
        [pos_ids // 256, pos_ids % 256, jnp.zeros((width - 2 * own,), jnp.int32)]
    ).astype(bf16)
    seen = jnp.concatenate([users, ids_row[None], jnp.zeros((block - own - 1, width), bf16)], 0)
    half_bank = jnp.concatenate([items, swap(items, "batch", 1)], 0)
    for bit, mask in steps:
        seen = doubled(seen, swap(seen, "items", mask), (here & bit) != 0)
    bank = jnp.concatenate([half_bank, swap(half_bank, "items", 1)], 0)
    rows = seen.shape[0]
    blocks = rows // block

    pairs = seen.reshape(blocks, block, width)[:, own, : 2 * own].astype(jnp.int32)
    ids = pairs[:, :own] * 256 + pairs[:, own:]
    owner = ids // per_bank
    at = owner % count
    slot = ((at ^ here) & 1) * 2 + ((owner // count) ^ group)
    column = jnp.where((at >> 1) == (here >> 1), slot * per_bank + ids % per_bank, -1)
    column = jnp.pad(column, ((0, 0), (0, block - own)), constant_values=-1).reshape(rows)
    cols = jnp.arange(bank.shape[0], dtype=jnp.int32)
    real = (jnp.arange(rows, dtype=jnp.int32) % block) < own

    logit = lax.dot_general(seen, bank, (((1,), (1,)), ((), ())), preferred_element_type=f32)
    match = column[:, None] == cols[None, :]
    peak = jnp.max(logit, axis=1)
    power = jnp.exp(logit - peak[:, None])
    total = jnp.sum(power, axis=1)
    positive = jnp.sum(jnp.where(match, logit, 0.0), axis=1)
    high = power.astype(bf16)
    low = (power - high.astype(f32)).astype(bf16)
    acc = jnp.dot(high, bank, preferred_element_type=f32) + jnp.dot(
        low, bank, preferred_element_type=f32
    )
    pick = jnp.dot(match.astype(bf16), bank, preferred_element_type=f32).astype(bf16)

    for bit, mask in reversed(steps):
        upper = ((here & bit) != 0).astype(jnp.int32)
        half = acc.shape[0] // 2
        stats = swap(jnp.stack([peak, total, positive]), "items", mask)
        give = (1 - upper) * half
        sent = jnp.concatenate(
            [
                lax.dynamic_slice_in_dim(acc, give, half, 0).astype(bf16),
                lax.dynamic_slice_in_dim(pick, give, half, 0),
            ],
            0,
        )
        got = swap(sent, "items", mask)
        top = jnp.maximum(peak, stats[0])
        scale_mine = jnp.exp(peak - top)
        scale_theirs = jnp.exp(stats[0] - top)
        total = total * scale_mine + stats[1] * scale_theirs
        positive = positive + stats[2]
        peak = top
        keep = upper * half
        base = keep if acc.shape[0] == rows else base + keep
        mine = lax.dynamic_slice_in_dim(scale_mine, base, half, 0)
        theirs = lax.dynamic_slice_in_dim(scale_theirs, base, half, 0)
        acc = (
            lax.dynamic_slice_in_dim(acc, keep, half, 0) * mine[:, None]
            + got[:half].astype(f32) * theirs[:, None]
        )
        pick = lax.dynamic_slice_in_dim(pick, keep, half, 0) + got[half:]

    lse = peak + jnp.log(total)
    last = lambda v: lax.dynamic_slice_in_dim(v, base, block, 0)[:own]
    loss = last(lse) - last(positive)
    user_grad = acc[:own] / last(total)[:, None] - pick[:own].astype(f32)

    weights = (jnp.exp(logit - lse[:, None]) - jnp.where(match, 1.0, 0.0)).astype(bf16)
    clean = jnp.where(real[:, None], seen, jnp.zeros((), bf16))
    grad = lax.dot_general(weights, clean, (((0,), (0,)), ((), ())), preferred_element_type=f32)
    near = 2 * per_bank
    grad = grad[:near] + swap(grad[near:], "items", 1)
    item_grad = grad[:per_bank] + swap(grad[per_bank:].astype(bf16), "batch", 1).astype(f32)
    return (loss, user_grad, item_grad)


def solution(mesh):
    placed = (P(("batch", "items"), None), P(("batch", "items"), None), P(("batch", "items")))
    return jax.shard_map(
        local,
        mesh=mesh,
        in_specs=placed,
        out_specs=(P(("batch", "items")), P(("batch", "items"), None), P(("batch", "items"), None)),
        check_vma=False,
    )
```

```python
import jax
import jax.numpy as jnp
from jax import lax
from jax.sharding import PartitionSpec as P


def swap(value, axis, mask):
    count = lax.axis_size(axis)
    return lax.ppermute(value, axis, [(i, i ^ mask) for i in range(count)])


def user_steps(count):
    bits = [1 << k for k in range(count.bit_length() - 1)][1:]
    steps = [(b, b) for b in bits[1:]]
    return steps + [(b, b) for b in bits[:1]]


def doubled(mine, theirs, upper):
    return jnp.where(
        upper, jnp.concatenate([theirs, mine], 0), jnp.concatenate([mine, theirs], 0)
    )


def local(users, items, pos_ids):
    f32, bf16 = jnp.float32, jnp.bfloat16
    own, width = users.shape
    per_bank = items.shape[0]
    count = lax.axis_size("items")
    here = lax.axis_index("items")
    group = lax.axis_index("batch")
    steps = user_steps(count)
    block = -(-(own + 1) // 16) * 16

    ids_row = jnp.concatenate(
        [pos_ids // 256, pos_ids % 256, jnp.zeros((width - 2 * own,), jnp.int32)]
    ).astype(bf16)
    seen = jnp.concatenate([users, ids_row[None], jnp.zeros((block - own - 1, width), bf16)], 0)
    half_bank = jnp.concatenate([items, swap(items, "batch", 1)], 0)
    for bit, mask in steps:
        theirs = swap(seen, "items", mask)
        seen = doubled(seen, theirs, (here & bit) != 0)
    bank = jnp.concatenate([half_bank, swap(half_bank, "items", 1)], 0)
    rows = seen.shape[0]
    blocks = rows // block

    pairs = seen.reshape(blocks, block, width)[:, own, : 2 * own].astype(jnp.int32)
    ids = pairs[:, :own] * 256 + pairs[:, own:]
    owner = ids // per_bank
    at = owner % count
    slot = ((at ^ here) & 1) * 2 + ((owner // count) ^ group)
    column = jnp.where((at >> 1) == (here >> 1), slot * per_bank + ids % per_bank, -1)
    column = jnp.pad(column, ((0, 0), (0, block - own)), constant_values=-1).reshape(rows)
    cols = jnp.arange(bank.shape[0], dtype=jnp.int32)
    real = (jnp.arange(rows, dtype=jnp.int32) % block) < own

    logit = lax.dot_general(seen, bank, (((1,), (1,)), ((), ())), preferred_element_type=f32)
    match = column[:, None] == cols[None, :]
    peak = jnp.max(logit, axis=1)
    power = jnp.exp(logit - peak[:, None])
    total = jnp.sum(power, axis=1)
    positive = jnp.sum(jnp.where(match, logit, 0.0), axis=1)
    high = power.astype(bf16)
    low = (power - high.astype(f32)).astype(bf16)
    acc = jnp.dot(high, bank, preferred_element_type=f32) + jnp.dot(
        low, bank, preferred_element_type=f32
    )
    pick = jnp.dot(match.astype(bf16), bank, preferred_element_type=f32).astype(bf16)

    for n, (bit, mask) in enumerate(reversed(steps)):
        upper = ((here & bit) != 0).astype(jnp.int32)
        half = acc.shape[0] // 2
        stats = swap(jnp.stack([peak, total, positive]), "items", mask)
        give = (1 - upper) * half
        wire = f32 if n == len(steps) - 1 else bf16
        sent = jnp.concatenate(
            [
                lax.dynamic_slice_in_dim(acc, give, half, 0).astype(wire),
                lax.dynamic_slice_in_dim(pick, give, half, 0).astype(wire),
            ],
            0,
        )
        got = swap(sent, "items", mask)
        top = jnp.maximum(peak, stats[0])
        scale_mine = jnp.exp(peak - top)
        scale_theirs = jnp.exp(stats[0] - top)
        total = total * scale_mine + stats[1] * scale_theirs
        positive = positive + stats[2]
        peak = top
        keep = upper * half
        base = keep if acc.shape[0] == rows else base + keep
        mine = lax.dynamic_slice_in_dim(scale_mine, base, half, 0)
        theirs = lax.dynamic_slice_in_dim(scale_theirs, base, half, 0)
        acc = (
            lax.dynamic_slice_in_dim(acc, keep, half, 0) * mine[:, None]
            + got[:half].astype(f32) * theirs[:, None]
        )
        pick = lax.dynamic_slice_in_dim(pick, keep, half, 0) + got[half:].astype(bf16)

    lse = peak + jnp.log(total)
    last = lambda v: lax.dynamic_slice_in_dim(v, base, block, 0)[:own]
    loss = last(lse) - last(positive)
    user_grad = acc[:own] / last(total)[:, None] - pick[:own].astype(f32)

    weights = (jnp.exp(logit - lse[:, None]) - jnp.where(match, 1.0, 0.0)).astype(bf16)
    clean = jnp.where(real[:, None], seen, jnp.zeros((), bf16))
    grad = lax.dot_general(weights, clean, (((0,), (0,)), ((), ())), preferred_element_type=f32)
    near = 2 * per_bank
    grad = grad[:near] + swap(grad[near:], "items", 1)
    item_grad = grad[:per_bank] + swap(grad[per_bank:].astype(bf16), "batch", 1).astype(f32)
    return (loss, user_grad, item_grad)


def solution(mesh):
    placed = (P(("batch", "items"), None), P(("batch", "items"), None), P(("batch", "items")))
    return jax.shard_map(
        local,
        mesh=mesh,
        in_specs=placed,
        out_specs=(P(("batch", "items")), P(("batch", "items"), None), P(("batch", "items"), None)),
        check_vma=False,
    )
```

```python
import jax
import jax.numpy as jnp
from jax import lax
from jax.sharding import PartitionSpec as P


def swap(value, axis, mask):
    count = lax.axis_size(axis)
    return lax.ppermute(value, axis, [(i, i ^ mask) for i in range(count)])


def user_steps(count):
    bits = [1 << k for k in range(count.bit_length() - 1)][1:]
    steps = [(b, b) for b in bits[1:]]
    return steps + [(b, b) for b in bits[:1]]


def doubled(mine, theirs, upper):
    return jnp.where(
        upper, jnp.concatenate([theirs, mine], 0), jnp.concatenate([mine, theirs], 0)
    )


def part(value, upper, size):
    return lax.dynamic_slice_in_dim(value, upper * size, size, 0)


def local(users, items, pos_ids):
    f32, bf16 = jnp.float32, jnp.bfloat16
    own, width = users.shape
    per_bank = items.shape[0]
    count = lax.axis_size("items")
    here = lax.axis_index("items")
    group = lax.axis_index("batch")
    steps = user_steps(count)
    block = -(-(own + 2) // 16) * 16

    ids_rows = jnp.stack([pos_ids // 256, pos_ids % 256])
    ids_rows = jnp.pad(ids_rows, ((0, block - own - 2), (0, width - own))).astype(bf16)
    seen = lax.optimization_barrier(jnp.concatenate([users, ids_rows], 0))
    half_bank = jnp.concatenate([items, swap(items, "batch", 1)], 0)
    for bit, mask in steps:
        theirs = swap(seen, "items", mask)
        seen = doubled(seen, theirs, (here & bit) != 0)
    bank = jnp.concatenate([half_bank, swap(half_bank, "items", 1)], 0)
    rows = seen.shape[0]
    blocks = rows // block

    pairs = seen.reshape(blocks, block, width)[:, own : own + 2, :own].astype(jnp.int32)
    ids = pairs[:, 0] * 256 + pairs[:, 1]
    owner = ids // per_bank
    at = owner % count
    slot = ((at ^ here) & 1) * 2 + ((owner // count) ^ group)
    column = jnp.where((at >> 1) == (here >> 1), slot * per_bank + ids % per_bank, -1)
    column = jnp.pad(column, ((0, 0), (0, block - own)), constant_values=-1).reshape(rows)
    cols = jnp.arange(bank.shape[0], dtype=jnp.int32)
    real = (jnp.arange(rows, dtype=jnp.int32) % block) < own

    logit = lax.dot_general(seen, bank, (((1,), (1,)), ((), ())), preferred_element_type=f32)
    match = column[:, None] == cols[None, :]
    peak = jnp.max(logit, axis=1)
    power = jnp.exp(logit - peak[:, None])
    total = jnp.sum(power, axis=1)
    positive = jnp.sum(jnp.where(match, logit, 0.0), axis=1)
    high = power.astype(bf16)
    low = (power - high.astype(f32)).astype(bf16)
    acc = jnp.dot(high, bank, preferred_element_type=f32) + jnp.dot(
        low, bank, preferred_element_type=f32
    )
    pick = jnp.dot(match.astype(bf16), bank, preferred_element_type=f32).astype(bf16)

    place = 0
    for n, (bit, mask) in enumerate(reversed(steps)):
        upper = ((here & bit) != 0).astype(jnp.int32)
        half = acc.shape[0] // 2
        stats = swap(jnp.stack([peak, total, positive]), "items", mask)
        wire = f32 if n == len(steps) - 1 else bf16
        sent = [part(acc, 1 - upper, half).astype(wire), part(pick, 1 - upper, half).astype(wire)]
        got = swap(jnp.concatenate(sent, 0), "items", mask)
        top = jnp.maximum(peak, stats[0])
        mine = jnp.exp(peak - top)
        theirs = jnp.exp(stats[0] - top)
        total = total * mine + stats[1] * theirs
        positive = positive + stats[2]
        peak = top
        mine, theirs, peak = lax.optimization_barrier((mine, theirs, peak))
        place = place * 2 + upper
        mine, theirs = part(mine, place, half), part(theirs, place, half)
        acc = part(acc, upper, half) * mine[:, None] + got[:half].astype(f32) * theirs[:, None]
        pick = part(pick, upper, half) + got[half:].astype(bf16)

    lse = peak + jnp.log(total)
    last = lambda value: part(value, place, block)[:own]
    loss = last(lse) - last(positive)
    user_grad = acc[:own] / last(total)[:, None] - pick[:own].astype(f32)

    weights = (jnp.exp(logit - lse[:, None]) - jnp.where(match, 1.0, 0.0)).astype(bf16)
    clean = jnp.where(real[:, None], seen, jnp.zeros((), bf16))
    grad = lax.dot_general(weights, clean, (((0,), (0,)), ((), ())), preferred_element_type=f32)
    near = 2 * per_bank
    grad = grad[:near] + swap(grad[near:], "items", 1)
    far = swap(grad[per_bank:].astype(bf16), "batch", 1)
    item_grad = grad[:per_bank] + far.astype(f32)
    return (loss, user_grad, item_grad)


def solution(mesh):
    placed = (P(("batch", "items"), None), P(("batch", "items"), None), P(("batch", "items")))
    return jax.shard_map(
        local,
        mesh=mesh,
        in_specs=placed,
        out_specs=(P(("batch", "items")), P(("batch", "items"), None), P(("batch", "items"), None)),
        check_vma=False,
    )
```
